128 devices in a mesh: tm: 2 (over z_hi), seq: 64 (over y, z_lo, x, core).
Axes of the slice: x: 4, y: 4, z: 4 (z_hi: 2, z_lo: 2; z = z_hi * 2 + z_lo), core: 2. Of those that a mesh axis runs over, the one named last changes fastest.
Arguments:
- tokens: bfloat16 [2048, 5120], P(('tm', 'seq')), may hold values from -6 to 6
- w_query: bfloat16 [5120, 4096], P('seq'), may hold values from -0.078125 to 0.078125
- w_out: bfloat16 [4096, 5120], P(None, 'seq'), may hold values from -0.25 to 0.25
- k_cache: bfloat16 [16384, 4096], P(('tm', 'seq')), may hold values from -800 to 800
- v_cache: bfloat16 [16384, 4096], P(('tm', 'seq')), may hold values from -6 to 6
- radial_mask: int32 [16, 8, 128], replicated, may hold values from 0 to 1, as said below
- slot_frame: int32 [16], replicated, may hold values from 0 to 15, each once
Outputs:
- mixed: bfloat16 [2048, 5120], P(('tm', 'seq'))
The draws below stay inside these ranges and needn't reach their ends.
Inputs may be any that keep to these rules, and one draw needn't show every extreme that they name: radial_mask[f, b, f * 8 + b] = 1 for every frame f and tile b. `slot_frame`: each of the 16 frames is held by exactly one slot.
All inputs are finite; a program needn't handle non-finite values.
Results may differ from the reference program's by a relative error of at most 0.012.
The reference program's roundings to bfloat16 on the way count: a program that leaves them out, or rounds other values in their place, can miss the bound.
Values may be sent and summed in bfloat16 or wider, within the bound.
No kernel may reach another device: no remote copies, remote signals or barrier semaphores. Data moves between devices by JAX's collectives and lax.ppermute only.
A program may use at most 128 MiB of HBM per device.

```python
import jax
import jax.numpy as jnp
from jax import lax

D = 5120
HD = 128
HEADS = 32
FRAMES = 16
BLOCK = 128
HH = 4096
FT = 1024
FB = 8
KEYS = 16384
N_TM = 2


def draw_k_cache(key, part):
    base = 2.5 * jnp.clip(jax.random.normal(jax.random.fold_in(key, 11), (KEYS, HEADS * HD), jnp.float32), -6.0, 6.0)
    return base.astype(jnp.bfloat16)


def draw_radial_mask(key, part):
    query_frame = jnp.arange(FRAMES, dtype=jnp.int32).reshape(FRAMES, 1, 1, 1)
    key_frame = jnp.arange(FRAMES, dtype=jnp.int32).reshape(1, 1, FRAMES, 1)
    query_block = jnp.arange(FB, dtype=jnp.int32).reshape(1, FB, 1, 1)
    key_block = jnp.arange(FB, dtype=jnp.int32).reshape(1, 1, 1, FB)
    distance = jnp.abs(query_frame - key_frame)
    band = jnp.zeros_like(distance)
    for level in range(1, 8):
        band = band + (distance + 1 >= 2 ** level).astype(jnp.int32)
    reach = jnp.maximum(jnp.right_shift(jnp.full_like(band, FB), band), 1)
    inside = jnp.abs(query_block - key_block) < reach
    kept = jax.random.randint(jax.random.fold_in(key, 21), (FRAMES, FB, FRAMES, FB), 0, 8) != 0
    diagonal = (distance == 0) & (query_block == key_block)
    mask = inside & kept | diagonal
    return mask.astype(jnp.int32).reshape(FRAMES, FB, FRAMES * FB)


def block_levels(stream_key, dims, pieces, least, largest):
    factor_of = 1.0
    for dim, shards_of in pieces:
        draws = jax.random.uniform(jax.random.fold_in(jax.random.fold_in(stream_key, 6), dim), (shards_of,), jnp.float32, least / len(pieces), largest / len(pieces))
        factor_of = factor_of * jnp.repeat(jnp.exp(draws), dims[dim] // shards_of).reshape((-1,) + (1,) * (len(dims) - 1 - dim))
    return factor_of


def gaussian(rng, shape, spread, bound, pieces=(), kind=jnp.bfloat16):
    drawn = spread * jax.random.normal(rng, shape, jnp.float32)
    if pieces:
        drawn = drawn * block_levels(rng, shape, pieces, -0.22, 0.18)
    return jnp.clip(drawn, -bound, bound).astype(kind)


def setup_inputs(seed: int = 0) -> dict:
    key_list = jax.random.split(jax.random.key(seed), 8)
    return {
        "tokens": gaussian(key_list[0], (N_TM * FT, D), 1.0, 6.0, ((0, 128),)),
        "w_query": gaussian(key_list[1], (D, HH), D ** -0.5, 0.078125, ((0, 64),)),
        "w_out": gaussian(key_list[2], (HH, D), (HH // 8) ** -0.5, 0.25, ((1, 64),)),
        "k_cache": draw_k_cache(jax.random.fold_in(key_list[7], 71), 0),
        "v_cache": gaussian(key_list[4], (KEYS, HH), 1.0, 6.0, ((0, 128),)),
        "radial_mask": draw_radial_mask(jax.random.fold_in(key_list[7], 71), 0),
        "slot_frame": jax.random.permutation(key_list[6], FRAMES).astype(jnp.int32),
    }


NEG = -1.0e30


def slot_allowed(radial_mask, slot_frame, frame):
    frame_blocks = radial_mask.shape[1]
    frames = slot_frame.shape[0]
    onehot = (slot_frame[:, None] == jnp.arange(frames, dtype=jnp.int32)[None, :]).astype(jnp.float32)
    chosen = lax.dynamic_index_in_dim(radial_mask, frame, 0, keepdims=False).astype(jnp.float32)
    chosen = chosen.reshape(frame_blocks, frames, frame_blocks)
    return jnp.einsum("sf,qfb->qsb", onehot, chosen).reshape(frame_blocks, frames * frame_blocks)


def reference(tokens, w_query, w_out, k_cache, v_cache, radial_mask, slot_frame):
    frame_tok = tokens.shape[0] // N_TM
    per_group = FRAMES // N_TM
    score_scale = HD ** -0.5
    key_heads = k_cache.reshape(-1, HEADS, HD).transpose(1, 0, 2)
    value_heads = v_cache.reshape(-1, HEADS, HD).transpose(1, 0, 2)
    results = []
    for group in range(N_TM):
        frame = slot_frame[group * per_group]
        allowed = slot_allowed(radial_mask, slot_frame, frame) > 0.5
        allowed = jnp.repeat(jnp.repeat(allowed, BLOCK, axis=0), BLOCK, axis=1)
        group_rows = tokens[group * frame_tok:(group + 1) * frame_tok]
        query = jnp.dot(group_rows, w_query, preferred_element_type=jnp.float32).astype(jnp.bfloat16)
        query_heads = query.reshape(frame_tok, HEADS, HD).transpose(1, 0, 2)

        def attend(operands):
            q_head, k_head, v_head = operands
            scores = jnp.dot(q_head, k_head.T, preferred_element_type=jnp.float32) * score_scale
            scores = jnp.where(allowed, scores, NEG)
            highest = jnp.max(scores, axis=1, keepdims=True)
            weights = jnp.where(allowed, jnp.exp(scores - highest), 0.0)
            denom = jnp.sum(weights, axis=1, keepdims=True)
            summed = jnp.dot(weights.astype(jnp.bfloat16), v_head, preferred_element_type=jnp.float32)
            return (summed / denom).astype(jnp.bfloat16)

        heads_out = lax.map(attend, (query_heads, key_heads, value_heads))
        attended = heads_out.transpose(1, 0, 2).reshape(frame_tok, HEADS * HD)
        results.append(jnp.dot(attended, w_out, preferred_element_type=jnp.float32).astype(jnp.bfloat16))
    return jnp.concatenate(results, axis=0)
```

```python
import functools
import math

import jax
import jax.numpy as jnp
from jax import lax
from jax.experimental import pallas as pl
from jax.experimental.pallas import tpu as pltpu
from jax.sharding import Mesh, PartitionSpec as P


HD = 128
HEADS = 32
BLOCK = 128
KEY_TILES = 32
GROUP = 8
Q_DEV = 16
NEG = -1e30
AXES = ("tm", "y", "zl", "x", "c")
PLANE = ("y", "x", "c")
NT = (((1,), (1,)), ((), ()))


def eye_mask():
    rows = lax.broadcasted_iota(jnp.int32, (BLOCK, BLOCK), 0)
    columns = lax.broadcasted_iota(jnp.int32, (BLOCK, BLOCK), 1)
    return rows == columns


def attention_kernel(place_ref, slot_ref, mask_ref, *refs):
    q_refs, kv_ref, o_ref = refs[:4], refs[4], refs[5]
    score_refs, high_refs, total_refs, sum_ref = refs[6:8], refs[8:10], refs[10:12], refs[12]
    scale = HD ** -0.5
    scale2 = scale * math.log2(math.e)
    plane = place_ref[0]

    def prepare(s):
        high_refs[s % 2][...] = jnp.full((4, BLOCK, BLOCK), NEG, jnp.float32)

    def score(s, t):
        source = lax.rem(plane - s + 4, 4)
        frame = slot_ref[lax.div(source, 2) * 8]
        q = q_refs[s][...]
        for pair in range(GROUP // 2):
            first = t * GROUP + pair * 2
            tiles = [kv_ref[first + u, :BLOCK] for u in range(2)]
            result = lax.dot_general(
                q, jnp.concatenate(tiles, 0), NT, preferred_element_type=jnp.float32
            )
            slot = lax.div(plane, 2) * 8 + lax.div(first, 8) * 2 + lax.rem(plane, 2)
            base = slot_ref[slot] * 8 + lax.rem(first, 8)
            for i in range(4):
                high = high_refs[s % 2][i]
                for u in range(2):
                    allowed = mask_ref[frame, 2 * i + lax.rem(source, 2), base + u] > 0
                    part = result[i * BLOCK : (i + 1) * BLOCK, u * BLOCK : (u + 1) * BLOCK]
                    part = jnp.where(allowed, part, NEG)
                    score_refs[s % 2][i, first + u] = part
                    high = jnp.maximum(high, part)
                high_refs[s % 2][i] = high

    def settle_high(s):
        for i in range(4):
            high = jnp.max(high_refs[s % 2][i], axis=1, keepdims=True)
            high_refs[s % 2][i] = jnp.broadcast_to(high, (BLOCK, BLOCK))
        total_refs[s % 2][...] = jnp.zeros((4, BLOCK, BLOCK), jnp.float32)
        sum_ref[...] = jnp.zeros((4 * BLOCK, HD), jnp.float32)

    def weigh(s, t):
        rows = []
        for i in range(4):
            high = high_refs[s % 2][i]
            total = total_refs[s % 2][i]
            parts = []
            for u in range(GROUP):
                w = jnp.exp2((score_refs[s % 2][i, t * GROUP + u] - high) * scale2)
                total = total + w
                parts.append(w.astype(jnp.bfloat16))
            total_refs[s % 2][i] = total
            rows.append(jnp.concatenate(parts, 1))
        values = jnp.concatenate([kv_ref[t * GROUP + u, BLOCK : 2 * BLOCK] for u in range(GROUP)], 0)
        sum_ref[...] += jnp.dot(jnp.concatenate(rows, 0), values, preferred_element_type=jnp.float32)

    def close(s):
        source = lax.rem(plane - s + 4, 4)
        pieces = []
        for i in range(4):
            denom = jnp.sum(total_refs[s % 2][i], axis=1, keepdims=True)
            high = jnp.max(high_refs[s % 2][i], axis=1, keepdims=True)
            done = (sum_ref[pl.ds(i * BLOCK, BLOCK), :] / denom).astype(jnp.bfloat16)
            for x in range(4):
                for core in range(2):
                    row = x * 32 + core * 16
                    o_ref[source * 2 + core, pl.ds(i * 64 + x * 16, 16), :] = done[row : row + 16]
            level = jnp.where(high > 0.5 * NEG, high * scale + jnp.log(denom), NEG)
            line = jnp.sum(jnp.where(eye_mask(), level, 0.0), axis=0, keepdims=True)
            first = line.astype(jnp.bfloat16)
            rest = line - first.astype(jnp.float32)
            second = rest.astype(jnp.bfloat16)
            third = (rest - second.astype(jnp.float32)).astype(jnp.bfloat16)
            pieces += [first, second, third]
        pieces.append(jnp.zeros((4, HD), jnp.bfloat16))
        for core in range(2):
            o_ref[source * 2 + core, pl.ds(256, 16), :] = jnp.concatenate(pieces, 0)

    def loop(body):
        def step(t, carry):
            body(t)
            return carry

        lax.fori_loop(0, KEY_TILES // GROUP, step, 0)

    prepare(0)
    loop(lambda t: score(0, t))
    for s in range(4):
        settle_high(s)
        if s < 3:
            prepare(s + 1)

        def step(t, s=s):
            weigh(s, t)
            if s < 3:
                score(s + 1, t)

        loop(step)
        close(s)


def attend(plane, slot_frame, radial_mask, queries, cache):
    vmem = pl.BlockSpec(memory_space=pltpu.VMEM)
    smem = pl.BlockSpec(memory_space=pltpu.SMEM)
    square = pltpu.VMEM((4, BLOCK, BLOCK), jnp.float32)
    scores = pltpu.VMEM((4, KEY_TILES, BLOCK, BLOCK), jnp.float32)
    return pl.pallas_call(
        attention_kernel,
        out_shape=jax.ShapeDtypeStruct((8, 272, HD), jnp.bfloat16),
        in_specs=[smem] * 3 + [vmem] * 5,
        out_specs=vmem,
        scratch_shapes=[scores] * 2 + [square] * 4 + [pltpu.VMEM((4 * BLOCK, HD), jnp.float32)],
        cost_estimate=pl.CostEstimate(
            flops=4 * 2048 * 4096 * HD, bytes_accessed=4 * 2**20, transcendentals=2048 * 4096
        ),
        name="attend",
    )(plane, slot_frame, radial_mask, *queries, cache)


def merge_kernel(core_ref, part_ref, out_ref):
    rows = lax.broadcasted_iota(jnp.int32, (64, BLOCK), 0)
    columns = lax.broadcasted_iota(jnp.int32, (64, BLOCK), 1)
    mine = columns == (rows // 16) * 32 + core_ref[0] * 16 + rows % 16
    for head in range(2):
        tails = [part_ref[2 * p + head, pl.ds(256, 16), :].astype(jnp.float32) for p in range(4)]
        for i in range(4):
            levels = [
                tail[3 * i : 3 * i + 1] + tail[3 * i + 1 : 3 * i + 2] + tail[3 * i + 2 : 3 * i + 3]
                for tail in tails
            ]
            high = functools.reduce(jnp.maximum, levels)
            shares = [jnp.exp(level - high) for level in levels]
            whole = functools.reduce(jnp.add, shares)
            summed = jnp.zeros((64, HD), jnp.float32)
            for p in range(4):
                column = jnp.sum(jnp.where(mine, shares[p] / whole, 0.0), axis=1, keepdims=True)
                part = part_ref[2 * p + head, pl.ds(i * 64, 64), :].astype(jnp.float32)
                summed = summed + part * column
            out_ref[pl.ds(i * 64, 64), head * HD : (head + 1) * HD] = summed.astype(jnp.bfloat16)


def merge(core, parts):
    vmem = pl.BlockSpec(memory_space=pltpu.VMEM)
    return pl.pallas_call(
        merge_kernel,
        out_shape=jax.ShapeDtypeStruct((256, 2 * HD), jnp.bfloat16),
        in_specs=[pl.BlockSpec(memory_space=pltpu.SMEM), vmem],
        out_specs=vmem,
        name="merge",
    )(core, parts)


def project_kernel(place_ref, *refs):
    rows, weights, outs, (w_ref, total_ref) = refs[:4], refs[4:6], refs[6:10], refs[10:]
    y, x, core = place_ref[0], place_ref[1], place_ref[2]
    size = weights[0].shape[0] // 8
    for side in range(2):
        for pair in range(8):
            block = pair * 2 + lax.rem(core + side, 2)
            target = pl.ds(pl.multiple_of(block * size, 16), size)
            w_ref[target, :] = weights[side][pl.ds(pair * size, size), :]
    total = None
    for s in range(4):
        source = lax.rem(y - s + 4, 4)
        w = w_ref[:, pl.ds(pl.multiple_of(source * 256, 256), 256)]
        term = lax.dot_general(rows[s][...], w, NT, preferred_element_type=jnp.float32)
        total = term if total is None else total + term
    total_ref[...] = total
    for s in range(4):
        target = lax.rem(x + s, 4)
        for i in range(4):
            start = pl.multiple_of(i * 64 + target * 16, 16)
            outs[s][pl.ds(i * 16, 16), :] = total_ref[pl.ds(start, 16), :].astype(outs[s].dtype)


def project(place, rows, weights):
    vmem = pl.BlockSpec(memory_space=pltpu.VMEM)
    kinds = [jnp.float32] + [jnp.bfloat16] * 3
    return pl.pallas_call(
        project_kernel,
        out_shape=tuple(jax.ShapeDtypeStruct((64, 1280), kind) for kind in kinds),
        in_specs=[pl.BlockSpec(memory_space=pltpu.SMEM)] + [vmem] * 6,
        out_specs=(vmem,) * 4,
        scratch_shapes=[
            pltpu.VMEM((1280, 8 * HD), jnp.bfloat16),
            pltpu.VMEM((256, 1280), jnp.float32),
        ],
        name="project",
    )(place, *rows, *weights)


def pack_query_kernel(place_ref, near_ref, far_ref, *out_refs):
    x, core = place_ref[1], place_ref[2]
    for s in range(4):
        for y in range(4):
            head = y * 8 + lax.rem(x + s, 4) * 2 + core
            columns = pl.ds(pl.multiple_of(head * HD, HD), HD)
            for side, w_ref in enumerate((near_ref, far_ref)):
                out_refs[s][side, :, y * HD : (y + 1) * HD] = w_ref[:, columns]


def pack_query(place, near, far):
    vmem = pl.BlockSpec(memory_space=pltpu.VMEM)
    rows = near.shape[0]
    return pl.pallas_call(
        pack_query_kernel,
        out_shape=(jax.ShapeDtypeStruct((2, rows, 4 * HD), jnp.bfloat16),) * 4,
        in_specs=[pl.BlockSpec(memory_space=pltpu.SMEM), vmem, vmem],
        out_specs=(vmem,) * 4,
        name="pack_query",
    )(place, near, far)


def pack_cache_kernel(k_ref, v_ref, out_ref):
    for head in range(HEADS):
        out_ref[head, :BLOCK, :] = k_ref[:, head * HD : (head + 1) * HD]
        out_ref[head, BLOCK:, :] = v_ref[:, head * HD : (head + 1) * HD]


def pack_cache(keys, values):
    vmem = pl.BlockSpec(memory_space=pltpu.VMEM)
    return pl.pallas_call(
        pack_cache_kernel,
        out_shape=jax.ShapeDtypeStruct((HEADS, 2 * BLOCK, HD), jnp.bfloat16),
        in_specs=[vmem, vmem],
        out_specs=vmem,
        name="pack_cache",
    )(keys, values)


def pack_tokens_kernel(token_ref, out_ref):
    width = out_ref.shape[2]
    for target in range(HEADS):
        column = target // 8 * width
        out_ref[target] = token_ref[:, column : column + width]


def pack_tokens(tokens):
    vmem = pl.BlockSpec(memory_space=pltpu.VMEM)
    return pl.pallas_call(
        pack_tokens_kernel,
        out_shape=jax.ShapeDtypeStruct((HEADS, Q_DEV, tokens.shape[1] // 4), jnp.bfloat16),
        in_specs=[vmem],
        out_specs=vmem,
        name="pack_tokens",
    )(tokens)


def settle_kernel(place_ref, *refs):
    parts, out_ref = refs[:4], refs[4]
    x = place_ref[1]
    size = parts[0].shape[1]
    for side in range(2):
        for s in range(4):
            block = side * 4 + lax.rem(x - s + 4, 4)
            out_ref[pl.ds(pl.multiple_of(block * size, 16), size), :] = parts[s][side]


def settle(place, parts):
    vmem = pl.BlockSpec(memory_space=pltpu.VMEM)
    _, rows, columns = parts[0].shape
    return pl.pallas_call(
        settle_kernel,
        out_shape=jax.ShapeDtypeStruct((8 * rows, columns), jnp.bfloat16),
        in_specs=[pl.BlockSpec(memory_space=pltpu.SMEM)] + [vmem] * 4,
        out_specs=vmem,
        name="settle",
    )(place, *parts)


def finish_kernel(place_ref, *refs):
    parts, out_ref = refs[:4], refs[4]
    width = parts[0].shape[1]
    for s in range(4):
        source = lax.rem(place_ref[0] - s + 4, 4)
        columns = pl.ds(pl.multiple_of(source * width, HD), width)
        out_ref[:, columns] = parts[s][...]


def finish(place, parts):
    vmem = pl.BlockSpec(memory_space=pltpu.VMEM)
    rows, width = parts[0].shape
    return pl.pallas_call(
        finish_kernel,
        out_shape=jax.ShapeDtypeStruct((rows, 4 * width), jnp.bfloat16),
        in_specs=[pl.BlockSpec(memory_space=pltpu.SMEM)] + [vmem] * 4,
        out_specs=vmem,
        name="finish",
    )(place, *parts)


def add_kernel(place_ref, *refs):
    parts, outs, total_ref = refs[:4], refs[4:8], refs[8]
    total = parts[0][...]
    for part in parts[1:]:
        total = total + part[...].astype(jnp.float32)
    total_ref[...] = total
    for s in range(4):
        start = pl.multiple_of(lax.rem(place_ref[0] + s, 4) * Q_DEV, Q_DEV)
        outs[s][...] = total_ref[pl.ds(start, Q_DEV), :].astype(jnp.bfloat16)


def add_parts(place, parts):
    vmem = pl.BlockSpec(memory_space=pltpu.VMEM)
    rows, width = parts[0].shape
    return pl.pallas_call(
        add_kernel,
        out_shape=(jax.ShapeDtypeStruct((Q_DEV, width), jnp.bfloat16),) * 4,
        in_specs=[pl.BlockSpec(memory_space=pltpu.SMEM)] + [vmem] * 4,
        out_specs=(vmem,) * 4,
        scratch_shapes=[pltpu.VMEM((rows, width), jnp.float32)],
        name="add_parts",
    )(place, *parts)


def pack_out_kernel(place_ref, *refs):
    x, zl = place_ref[1], place_ref[3]
    halves, out_refs = refs[:4], refs[4:]
    for s in range(4):
        for z_side in range(2):
            side = lax.rem(zl + z_side, 2)
            for y in range(4):
                head = y % 2 * 8 + lax.rem(x + s, 4) * 2
                columns = pl.ds(pl.multiple_of(head * HD, 2 * HD), 2 * HD)
                block = halves[z_side * 2 + y // 2][:, columns]
                out_refs[s][side, :, y * 2 * HD : (y + 1) * 2 * HD] = block


def pack_out(place, halves):
    vmem = pl.BlockSpec(memory_space=pltpu.VMEM)
    rows = halves[0].shape[0]
    return pl.pallas_call(
        pack_out_kernel,
        out_shape=(jax.ShapeDtypeStruct((2, rows, 8 * HD), jnp.bfloat16),) * 4,
        in_specs=[pl.BlockSpec(memory_space=pltpu.SMEM)] + [vmem] * 4,
        out_specs=(vmem,) * 4,
        name="pack_out",
    )(place, *halves)


def query_kernel(place_ref, token_ref, *refs):
    weights, out_refs, (w_ref, total_ref) = refs[:8], refs[8:12], refs[12:]
    y, x, core, zl = place_ref[0], place_ref[1], place_ref[2], place_ref[3]
    size = weights[0].shape[1]
    for z_side in range(2):
        for side in range(2):
            for s in range(4):
                block = lax.rem(zl + z_side, 2) * 8 + lax.rem(x - s + 4, 4) * 2
                block = block + lax.rem(core + side, 2)
                rows = pl.ds(pl.multiple_of(block * size, 16), size)
                w_ref[rows, :] = weights[z_side * 4 + s][side]
    total_ref[...] = jnp.dot(token_ref[...], w_ref[...], preferred_element_type=jnp.float32)
    for s in range(4):
        columns = pl.ds(pl.multiple_of(lax.rem(y + s, 4) * HD, HD), HD)
        out_refs[s][...] = total_ref[:, columns]


def query_parts(place, token_rows, weights):
    vmem = pl.BlockSpec(memory_space=pltpu.VMEM)
    rows, depth = token_rows.shape
    return pl.pallas_call(
        query_kernel,
        out_shape=(jax.ShapeDtypeStruct((rows, HD), jnp.float32),) * 4,
        in_specs=[pl.BlockSpec(memory_space=pltpu.SMEM)] + [vmem] * 9,
        out_specs=(vmem,) * 4,
        scratch_shapes=[
            pltpu.VMEM((depth, 4 * HD), jnp.bfloat16),
            pltpu.VMEM((rows, 4 * HD), jnp.float32),
        ],
        cost_estimate=pl.CostEstimate(
            flops=2 * rows * depth * 4 * HD, bytes_accessed=4 * 2**20, transcendentals=0
        ),
        name="query_parts",
    )(place, token_rows, *weights)


def z_shift(value, shift):
    return lax.ppermute(value, ("tm", "zl"), [(i, (i + shift) % 4) for i in range(4)])


def ring_shift(value, axis, shift):
    return lax.ppermute(value, axis, [(i, (i + shift) % 4) for i in range(4)])


def core_swap(value):
    return lax.ppermute(value, "c", [(0, 1), (1, 0)])


def exchange(table, axes):
    return lax.all_to_all(table, axes, split_axis=0, concat_axis=0, tiled=True)


def on_device(tokens, w_query, w_out, k_cache, v_cache, radial_mask, slot_frame):
    plane = (lax.axis_index("tm") * 2 + lax.axis_index("zl")).reshape(1)
    core = lax.axis_index("c").reshape(1)
    place = jnp.stack([lax.axis_index(a) for a in ("y", "x", "c", "zl")])

    packed = pack_query(place, w_query, core_swap(w_query))
    got = [packed[0]] + [ring_shift(packed[s], "x", s) for s in (1, 2, 3)]
    weights = got + [z_shift(got[s], 1) for s in (0, 1)] + [z_shift(got[s], -1) for s in (2, 3)]

    token_rows = exchange(pack_tokens(tokens), PLANE)

    half = w_out.shape[0] // 2
    low, high = w_out[:half].T, w_out[half:].T
    packed_out = pack_out(place, (low, high, z_shift(low, 1), z_shift(high, -1)))
    cache = pack_cache(k_cache, v_cache)
    ready = lax.optimization_barrier((weights, packed_out, cache, token_rows))
    weights, packed_out, cache, token_rows = ready

    partial = query_parts(place, token_rows.reshape(-1, token_rows.shape[2]), weights)
    partial, cache, packed_out = lax.optimization_barrier((partial, cache, packed_out))
    partial = [partial[0]] + [ring_shift(partial[s], "y", s) for s in (1, 2, 3)]
    arrived = exchange(cache, PLANE)
    got = [packed_out[0]] + [ring_shift(packed_out[s], "x", s) for s in (1, 2, 3)]

    query = functools.reduce(jnp.add, partial).astype(jnp.bfloat16)
    queries = [query] + [z_shift(query, s) for s in (1, 2, 3)]
    outs = attend(plane, slot_frame, radial_mask, queries, arrived)

    got, outs = lax.optimization_barrier((got, outs))
    out_near = settle(place, got)
    out_far = core_swap(out_near)
    parts = exchange(outs, ("tm", "zl", "c"))
    attended = merge(core, parts)
    rows = [attended] + [ring_shift(attended, "y", s) for s in (1, 2, 3)]
    parts = project(place, rows, (out_near, out_far))
    parts = [parts[0]] + [ring_shift(parts[s], "x", s) for s in (1, 2, 3)]
    parts = add_parts(place, parts)
    parts = [parts[0]] + [ring_shift(parts[s], "y", s) for s in (1, 2, 3)]
    return finish(place, parts)


def solution(mesh):
    fine = Mesh(mesh.devices.reshape(2, 4, 2, 4, 2), AXES)
    return jax.shard_map(
        on_device,
        mesh=fine,
        in_specs=(
            P(AXES, None),
            P(("y", "zl", "x", "c"), None),
            P(None, ("y", "zl", "x", "c")),
            P(AXES, None),
            P(AXES, None),
            P(),
            P(),
        ),
        out_specs=P(AXES, None),
        check_vma=False,
    )
```

```python
import functools
import math

import jax
import jax.numpy as jnp
from jax import lax
from jax.experimental import pallas as pl
from jax.experimental.pallas import tpu as pltpu
from jax.sharding import Mesh, PartitionSpec as P


HD = 128
HEADS = 32
BLOCK = 128
KEY_TILES = 32
GROUP = 16
Q_DEV = 16
NEG = -1e30
AXES = ("tm", "y", "zl", "x", "c")
PLANE = ("y", "x", "c")
NT = (((1,), (1,)), ((), ()))


def eye_mask():
    rows = lax.broadcasted_iota(jnp.int32, (BLOCK, BLOCK), 0)
    columns = lax.broadcasted_iota(jnp.int32, (BLOCK, BLOCK), 1)
    return rows == columns


def attention_kernel(place_ref, slot_ref, mask_ref, *refs):
    q_refs, kv_ref, o_ref = refs[:4], refs[4], refs[5]
    score_refs, high_refs, total_refs, sum_ref = refs[6:8], refs[8:10], refs[10:12], refs[12]
    scale = HD ** -0.5
    scale2 = scale * math.log2(math.e)
    plane = place_ref[0]

    def prepare(s):
        high_refs[s % 2][...] = jnp.full((4, BLOCK, BLOCK), NEG, jnp.float32)

    def score(s, t):
        source = lax.rem(plane - s + 4, 4)
        frame = slot_ref[lax.div(source, 2) * 8]
        q = q_refs[s][...]
        for pair in range(GROUP // 2):
            first = t * GROUP + pair * 2
            tiles = [kv_ref[first + u, :BLOCK] for u in range(2)]
            result = lax.dot_general(
                q, jnp.concatenate(tiles, 0), NT, preferred_element_type=jnp.float32
            )
            slot = lax.div(plane, 2) * 8 + lax.div(first, 8) * 2 + lax.rem(plane, 2)
            base = slot_ref[slot] * 8 + lax.rem(first, 8)
            for i in range(4):
                high = high_refs[s % 2][i]
                for u in range(2):
                    allowed = mask_ref[frame, 2 * i + lax.rem(source, 2), base + u] > 0
                    part = result[i * BLOCK : (i + 1) * BLOCK, u * BLOCK : (u + 1) * BLOCK]
                    part = jnp.where(allowed, part, NEG)
                    score_refs[s % 2][i, first + u] = part
                    high = jnp.maximum(high, part)
                high_refs[s % 2][i] = high

    def settle_high(s):
        for i in range(4):
            high = jnp.max(high_refs[s % 2][i], axis=1, keepdims=True)
            high_refs[s % 2][i] = jnp.broadcast_to(high, (BLOCK, BLOCK))
        total_refs[s % 2][...] = jnp.zeros((4, BLOCK, BLOCK), jnp.float32)
        sum_ref[...] = jnp.zeros((4 * BLOCK, HD), jnp.float32)

    def weigh(s, t):
        rows = []
        for i in range(4):
            high = high_refs[s % 2][i]
            total = total_refs[s % 2][i]
            parts = []
            for u in range(GROUP):
                w = jnp.exp2((score_refs[s % 2][i, t * GROUP + u] - high) * scale2)
                total = total + w
                parts.append(w.astype(jnp.bfloat16))
            total_refs[s % 2][i] = total
            rows.append(jnp.concatenate(parts, 1))
        values = jnp.concatenate([kv_ref[t * GROUP + u, BLOCK : 2 * BLOCK] for u in range(GROUP)], 0)
        sum_ref[...] += jnp.dot(jnp.concatenate(rows, 0), values, preferred_element_type=jnp.float32)

    def close(s):
        source = lax.rem(plane - s + 4, 4)
        pieces = []
        for i in range(4):
            denom = jnp.sum(total_refs[s % 2][i], axis=1, keepdims=True)
            high = jnp.max(high_refs[s % 2][i], axis=1, keepdims=True)
            done = (sum_ref[pl.ds(i * BLOCK, BLOCK), :] / denom).astype(jnp.bfloat16)
            for x in range(4):
                for core in range(2):
                    row = x * 32 + core * 16
                    o_ref[source * 2 + core, pl.ds(i * 64 + x * 16, 16), :] = done[row : row + 16]
            level = jnp.where(high > 0.5 * NEG, high * scale + jnp.log(denom), NEG)
            line = jnp.sum(jnp.where(eye_mask(), level, 0.0), axis=0, keepdims=True)
            first = line.astype(jnp.bfloat16)
            rest = line - first.astype(jnp.float32)
            second = rest.astype(jnp.bfloat16)
            third = (rest - second.astype(jnp.float32)).astype(jnp.bfloat16)
            pieces += [first, second, third]
        pieces.append(jnp.zeros((4, HD), jnp.bfloat16))
        for core in range(2):
            o_ref[source * 2 + core, pl.ds(256, 16), :] = jnp.concatenate(pieces, 0)

    def loop(body):
        def step(t, carry):
            body(t)
            return carry

        lax.fori_loop(0, KEY_TILES // GROUP, step, 0)

    prepare(0)
    loop(lambda t: score(0, t))
    for s in range(4):
        settle_high(s)
        if s < 3:
            prepare(s + 1)

        def step(t, s=s):
            weigh(s, t)
            if s < 3:
                score(s + 1, t)

        loop(step)
        close(s)


def attend(plane, slot_frame, radial_mask, queries, cache):
    vmem = pl.BlockSpec(memory_space=pltpu.VMEM)
    smem = pl.BlockSpec(memory_space=pltpu.SMEM)
    square = pltpu.VMEM((4, BLOCK, BLOCK), jnp.float32)
    scores = pltpu.VMEM((4, KEY_TILES, BLOCK, BLOCK), jnp.float32)
    return pl.pallas_call(
        attention_kernel,
        out_shape=jax.ShapeDtypeStruct((8, 272, HD), jnp.bfloat16),
        in_specs=[smem] * 3 + [vmem] * 5,
        out_specs=vmem,
        scratch_shapes=[scores] * 2 + [square] * 4 + [pltpu.VMEM((4 * BLOCK, HD), jnp.float32)],
        cost_estimate=pl.CostEstimate(
            flops=4 * 2048 * 4096 * HD, bytes_accessed=4 * 2**20, transcendentals=2048 * 4096
        ),
        name="attend",
    )(plane, slot_frame, radial_mask, *queries, cache)


def merge_kernel(core_ref, part_ref, out_ref):
    rows = lax.broadcasted_iota(jnp.int32, (64, BLOCK), 0)
    columns = lax.broadcasted_iota(jnp.int32, (64, BLOCK), 1)
    mine = columns == (rows // 16) * 32 + core_ref[0] * 16 + rows % 16
    for head in range(2):
        tails = [part_ref[2 * p + head, pl.ds(256, 16), :].astype(jnp.float32) for p in range(4)]
        for i in range(4):
            levels = [
                tail[3 * i : 3 * i + 1] + tail[3 * i + 1 : 3 * i + 2] + tail[3 * i + 2 : 3 * i + 3]
                for tail in tails
            ]
            high = functools.reduce(jnp.maximum, levels)
            shares = [jnp.exp(level - high) for level in levels]
            whole = functools.reduce(jnp.add, shares)
            summed = jnp.zeros((64, HD), jnp.float32)
            for p in range(4):
                column = jnp.sum(jnp.where(mine, shares[p] / whole, 0.0), axis=1, keepdims=True)
                part = part_ref[2 * p + head, pl.ds(i * 64, 64), :].astype(jnp.float32)
                summed = summed + part * column
            out_ref[pl.ds(i * 64, 64), head * HD : (head + 1) * HD] = summed.astype(jnp.bfloat16)


def merge(core, parts):
    vmem = pl.BlockSpec(memory_space=pltpu.VMEM)
    return pl.pallas_call(
        merge_kernel,
        out_shape=jax.ShapeDtypeStruct((256, 2 * HD), jnp.bfloat16),
        in_specs=[pl.BlockSpec(memory_space=pltpu.SMEM), vmem],
        out_specs=vmem,
        name="merge",
    )(core, parts)


def project_kernel(place_ref, *refs):
    rows, w_ref, out_ref = refs[:4], refs[4], refs[5]
    total = None
    for s in range(4):
        source = lax.rem(place_ref[0] - s + 4, 4)
        w = w_ref[:, pl.ds(pl.multiple_of(source * 256, 256), 256)]
        term = lax.dot_general(rows[s][...], w, NT, preferred_element_type=jnp.float32)
        total = term if total is None else total + term
    for target in range(16):
        out_ref[target] = total[target * Q_DEV : (target + 1) * Q_DEV].astype(jnp.bfloat16)


def project(place, rows, weights):
    vmem = pl.BlockSpec(memory_space=pltpu.VMEM)
    width = weights.shape[0]
    return pl.pallas_call(
        project_kernel,
        out_shape=jax.ShapeDtypeStruct((16, Q_DEV, width), jnp.bfloat16),
        in_specs=[pl.BlockSpec(memory_space=pltpu.SMEM)] + [vmem] * 5,
        out_specs=vmem,
        name="project",
    )(place, *rows, weights)


def pack_query_kernel(place_ref, near_ref, far_ref, *out_refs):
    x, core = place_ref[1], place_ref[2]
    for s in range(4):
        for y in range(4):
            head = y * 8 + lax.rem(x + s, 4) * 2 + core
            columns = pl.ds(pl.multiple_of(head * HD, HD), HD)
            for side, w_ref in enumerate((near_ref, far_ref)):
                out_refs[s][side, :, y * HD : (y + 1) * HD] = w_ref[:, columns]


def pack_query(place, near, far):
    vmem = pl.BlockSpec(memory_space=pltpu.VMEM)
    rows = near.shape[0]
    return pl.pallas_call(
        pack_query_kernel,
        out_shape=(jax.ShapeDtypeStruct((2, rows, 4 * HD), jnp.bfloat16),) * 4,
        in_specs=[pl.BlockSpec(memory_space=pltpu.SMEM), vmem, vmem],
        out_specs=(vmem,) * 4,
        name="pack_query",
    )(place, near, far)


def pack_cache_kernel(k_ref, v_ref, out_ref):
    for head in range(HEADS):
        out_ref[head, :BLOCK, :] = k_ref[:, head * HD : (head + 1) * HD]
        out_ref[head, BLOCK:, :] = v_ref[:, head * HD : (head + 1) * HD]


def pack_cache(keys, values):
    vmem = pl.BlockSpec(memory_space=pltpu.VMEM)
    return pl.pallas_call(
        pack_cache_kernel,
        out_shape=jax.ShapeDtypeStruct((HEADS, 2 * BLOCK, HD), jnp.bfloat16),
        in_specs=[vmem, vmem],
        out_specs=vmem,
        name="pack_cache",
    )(keys, values)


def pack_tokens_kernel(token_ref, out_ref):
    width = out_ref.shape[2]
    for target in range(HEADS):
        column = target // 8 * width
        out_ref[target] = token_ref[:, column : column + width]


def pack_tokens(tokens):
    vmem = pl.BlockSpec(memory_space=pltpu.VMEM)
    return pl.pallas_call(
        pack_tokens_kernel,
        out_shape=jax.ShapeDtypeStruct((HEADS, Q_DEV, tokens.shape[1] // 4), jnp.bfloat16),
        in_specs=[vmem],
        out_specs=vmem,
        name="pack_tokens",
    )(tokens)


def settle_kernel(place_ref, *refs):
    parts, out_ref = refs[:8], refs[8]
    x, zl = place_ref[1], place_ref[3]
    size = parts[0].shape[0]
    for z_side in range(2):
        for s in range(4):
            block = lax.rem(zl + z_side, 2) * 4 + lax.rem(x - s + 4, 4)
            out_ref[pl.ds(pl.multiple_of(block * size, 16), size), :] = parts[z_side * 4 + s][...]


def settle(place, parts):
    vmem = pl.BlockSpec(memory_space=pltpu.VMEM)
    rows, columns = parts[0].shape
    return pl.pallas_call(
        settle_kernel,
        out_shape=jax.ShapeDtypeStruct((8 * rows, columns), jnp.bfloat16),
        in_specs=[pl.BlockSpec(memory_space=pltpu.SMEM)] + [vmem] * 8,
        out_specs=vmem,
        name="settle",
    )(place, *parts)


def finish_kernel(part_ref, out_ref):
    width = part_ref.shape[2]
    for y in range(4):
        parts = [part_ref[y * 4 + x].astype(jnp.float32) for x in range(4)]
        total = functools.reduce(jnp.add, parts)
        out_ref[:, y * width : (y + 1) * width] = total.astype(jnp.bfloat16)


def finish(parts):
    vmem = pl.BlockSpec(memory_space=pltpu.VMEM)
    _, rows, width = parts.shape
    return pl.pallas_call(
        finish_kernel,
        out_shape=jax.ShapeDtypeStruct((rows, 4 * width), jnp.bfloat16),
        in_specs=[vmem],
        out_specs=vmem,
        name="finish",
    )(parts)


def pack_out_kernel(place_ref, w_ref, *out_refs):
    x = place_ref[1]
    for s in range(4):
        for y in range(4):
            head = y * 8 + lax.rem(x + s, 4) * 2
            columns = pl.ds(pl.multiple_of(head * HD, 2 * HD), 2 * HD)
            out_refs[s][:, y * 2 * HD : (y + 1) * 2 * HD] = w_ref[:, columns]


def pack_out(place, table):
    vmem = pl.BlockSpec(memory_space=pltpu.VMEM)
    rows = table.shape[0]
    return pl.pallas_call(
        pack_out_kernel,
        out_shape=(jax.ShapeDtypeStruct((rows, 8 * HD), jnp.bfloat16),) * 4,
        in_specs=[pl.BlockSpec(memory_space=pltpu.SMEM), vmem],
        out_specs=(vmem,) * 4,
        name="pack_out",
    )(place, table)


def weave_query_kernel(place_ref, *refs):
    weights, out_ref = refs[:8], refs[8]
    y, x, core, zl = place_ref[0], place_ref[1], place_ref[2], place_ref[3]
    size = weights[0].shape[1]
    for z_side in range(2):
        for side in range(2):
            for s in range(4):
                block = lax.rem(zl + z_side, 2) * 8 + lax.rem(x - s + 4, 4) * 2
                block = block + lax.rem(core + side, 2)
                rows = pl.ds(pl.multiple_of(block * size, 16), size)
                for t in range(4):
                    columns = pl.ds(pl.multiple_of(lax.rem(y + t, 4) * HD, HD), HD)
                    block = weights[z_side * 4 + s][side, :, columns]
                    out_ref[rows, t * HD : (t + 1) * HD] = block


def weave_query(place, weights):
    vmem = pl.BlockSpec(memory_space=pltpu.VMEM)
    _, rows, columns = weights[0].shape
    return pl.pallas_call(
        weave_query_kernel,
        out_shape=jax.ShapeDtypeStruct((16 * rows, columns), jnp.bfloat16),
        in_specs=[pl.BlockSpec(memory_space=pltpu.SMEM)] + [vmem] * 8,
        out_specs=vmem,
        name="weave_query",
    )(place, *weights)


def weave_out_kernel(place_ref, *refs):
    weights, out_ref = refs[:2], refs[2]
    core = place_ref[2]
    size = weights[0].shape[0] // 8
    for side in range(2):
        for pair in range(8):
            block = pair * 2 + lax.rem(core + side, 2)
            target = pl.ds(pl.multiple_of(block * size, 16), size)
            out_ref[target, :] = weights[side][pl.ds(pair * size, size), :]


def weave_out(place, weights):
    vmem = pl.BlockSpec(memory_space=pltpu.VMEM)
    rows, columns = weights[0].shape
    return pl.pallas_call(
        weave_out_kernel,
        out_shape=jax.ShapeDtypeStruct((2 * rows, columns), jnp.bfloat16),
        in_specs=[pl.BlockSpec(memory_space=pltpu.SMEM)] + [vmem] * 2,
        out_specs=vmem,
        name="weave_out",
    )(place, *weights)


def query_kernel(token_ref, w_ref, *out_refs):
    for pair in range(2):
        w = w_ref[:, pair * 2 * HD : (pair + 1) * 2 * HD]
        total = jnp.dot(token_ref[...], w, preferred_element_type=jnp.float32)
        out_refs[2 * pair][...] = total[:, :HD]
        out_refs[2 * pair + 1][...] = total[:, HD:]


def query_parts(token_rows, weights):
    vmem = pl.BlockSpec(memory_space=pltpu.VMEM)
    rows, depth = token_rows.shape
    return pl.pallas_call(
        query_kernel,
        out_shape=(jax.ShapeDtypeStruct((rows, HD), jnp.float32),) * 4,
        in_specs=[vmem] * 2,
        out_specs=(vmem,) * 4,
        cost_estimate=pl.CostEstimate(
            flops=2 * rows * depth * 4 * HD, bytes_accessed=4 * 2**20, transcendentals=0
        ),
        name="query_parts",
    )(token_rows, weights)


def z_shift(value, shift):
    return lax.ppermute(value, ("tm", "zl"), [(i, (i + shift) % 4) for i in range(4)])


def ring_shift(value, axis, shift):
    return lax.ppermute(value, axis, [(i, (i + shift) % 4) for i in range(4)])


def core_swap(value):
    return lax.ppermute(value, "c", [(0, 1), (1, 0)])


def exchange(table, axes):
    return lax.all_to_all(table, axes, split_axis=0, concat_axis=0, tiled=True)


def on_device(tokens, w_query, w_out, k_cache, v_cache, radial_mask, slot_frame):
    plane = (lax.axis_index("tm") * 2 + lax.axis_index("zl")).reshape(1)
    core = lax.axis_index("c").reshape(1)
    place = jnp.stack([lax.axis_index(a) for a in ("y", "x", "c", "zl")])

    packed = pack_query(place, w_query, core_swap(w_query))
    got = [packed[0]] + [ring_shift(packed[s], "x", s) for s in (1, 2, 3)]
    weights = got + [z_shift(got[s], 1) for s in (0, 1)] + [z_shift(got[s], -1) for s in (2, 3)]

    token_rows = exchange(pack_tokens(tokens), PLANE)

    packed_out = pack_out(place, w_out.T)
    got_out = [packed_out[0]] + [ring_shift(packed_out[s], "x", s) for s in (1, 2, 3)]

    cache = pack_cache(k_cache, v_cache)
    weights = weave_query(place, weights)
    weights, cache, token_rows = lax.optimization_barrier((weights, cache, token_rows))

    partial = query_parts(token_rows.reshape(-1, token_rows.shape[2]), weights)
    partial, cache, got_out = lax.optimization_barrier((partial, cache, got_out))
    partial = [partial[0]] + [ring_shift(partial[s], "y", s) for s in (1, 2, 3)]
    arrived = exchange(cache, PLANE)
    got_out = list(got_out)
    got_out += [z_shift(got_out[s], 1) for s in (0, 1)]
    got_out += [z_shift(got_out[s], -1) for s in (2, 3)]

    query = functools.reduce(jnp.add, partial).astype(jnp.bfloat16)
    queries = [query] + [z_shift(query, s) for s in (1, 2, 3)]
    outs = attend(plane, slot_frame, radial_mask, queries, arrived)

    got_out, outs = lax.optimization_barrier((got_out, outs))
    out_near = settle(place, got_out)
    parts = exchange(outs, ("tm", "zl", "c"))
    out_far = core_swap(out_near)
    out_weights = weave_out(place, (out_near, out_far))
    attended = merge(core, parts)
    rows = [attended] + [ring_shift(attended, "y", s) for s in (1, 2, 3)]
    return finish(exchange(project(place, rows, out_weights), ("y", "x")))


def solution(mesh):
    fine = Mesh(mesh.devices.reshape(2, 4, 2, 4, 2), AXES)
    return jax.shard_map(
        on_device,
        mesh=fine,
        in_specs=(
            P(AXES, None),
            P(("y", "zl", "x", "c"), None),
            P(None, ("y", "zl", "x", "c")),
            P(AXES, None),
            P(AXES, None),
            P(),
            P(),
        ),
        out_specs=P(AXES, None),
        check_vma=False,
    )
```

```python
import functools
import math

import jax
import jax.numpy as jnp
from jax import lax
from jax.experimental import pallas as pl
from jax.experimental.pallas import tpu as pltpu
from jax.sharding import Mesh, PartitionSpec as P


HD = 128
HEADS = 32
BLOCK = 128
KEY_TILES = 32
GROUP = 16
Q_DEV = 16
NEG = -1e30
AXES = ("tm", "y", "zl", "x", "c")
PLANE = ("y", "x", "c")
NT = (((1,), (1,)), ((), ()))


def eye_mask():
    rows = lax.broadcasted_iota(jnp.int32, (BLOCK, BLOCK), 0)
    columns = lax.broadcasted_iota(jnp.int32, (BLOCK, BLOCK), 1)
    return rows == columns


def attention_kernel(place_ref, slot_ref, mask_ref, *refs):
    q_refs, kv_ref, o_ref = refs[:4], refs[4], refs[5]
    score_refs, high_refs, total_refs, sum_ref = refs[6:8], refs[8:10], refs[10:12], refs[12]
    scale = HD ** -0.5
    scale2 = scale * math.log2(math.e)
    plane = place_ref[0]

    def prepare(s):
        high_refs[s % 2][...] = jnp.full((4, BLOCK, BLOCK), NEG, jnp.float32)

    def score(s, t):
        source = lax.rem(plane - s + 4, 4)
        frame = slot_ref[lax.div(source, 2) * 8]
        q = q_refs[s][...]
        for pair in range(GROUP // 2):
            first = t * GROUP + pair * 2
            tiles = [kv_ref[first + u, :BLOCK] for u in range(2)]
            result = lax.dot_general(
                q, jnp.concatenate(tiles, 0), NT, preferred_element_type=jnp.float32
            )
            slot = lax.div(plane, 2) * 8 + lax.div(first, 8) * 2 + lax.rem(plane, 2)
            base = slot_ref[slot] * 8 + lax.rem(first, 8)
            for i in range(4):
                high = high_refs[s % 2][i]
                for u in range(2):
                    allowed = mask_ref[frame, 2 * i + lax.rem(source, 2), base + u] > 0
                    part = result[i * BLOCK : (i + 1) * BLOCK, u * BLOCK : (u + 1) * BLOCK]
                    part = jnp.where(allowed, part, NEG)
                    score_refs[s % 2][i, first + u] = part
                    high = jnp.maximum(high, part)
                high_refs[s % 2][i] = high

    def settle_high(s):
        for i in range(4):
            high = jnp.max(high_refs[s % 2][i], axis=1, keepdims=True)
            high_refs[s % 2][i] = jnp.broadcast_to(high, (BLOCK, BLOCK))
        total_refs[s % 2][...] = jnp.zeros((4, BLOCK, BLOCK), jnp.float32)
        sum_ref[...] = jnp.zeros((4 * BLOCK, HD), jnp.float32)

    def weigh(s, t):
        rows = []
        for i in range(4):
            high = high_refs[s % 2][i]
            total = total_refs[s % 2][i]
            parts = []
            for u in range(GROUP):
                w = jnp.exp2((score_refs[s % 2][i, t * GROUP + u] - high) * scale2)
                total = total + w
                parts.append(w.astype(jnp.bfloat16))
            total_refs[s % 2][i] = total
            rows.append(jnp.concatenate(parts, 1))
        values = jnp.concatenate([kv_ref[t * GROUP + u, BLOCK : 2 * BLOCK] for u in range(GROUP)], 0)
        sum_ref[...] += jnp.dot(jnp.concatenate(rows, 0), values, preferred_element_type=jnp.float32)

    def close(s):
        source = lax.rem(plane - s + 4, 4)
        pieces = []
        for i in range(4):
            denom = jnp.sum(total_refs[s % 2][i], axis=1, keepdims=True)
            high = jnp.max(high_refs[s % 2][i], axis=1, keepdims=True)
            done = (sum_ref[pl.ds(i * BLOCK, BLOCK), :] / denom).astype(jnp.bfloat16)
            for x in range(4):
                for core in range(2):
                    row = x * 32 + core * 16
                    o_ref[source * 2 + core, pl.ds(i * 64 + x * 16, 16), :] = done[row : row + 16]
            level = jnp.where(high > 0.5 * NEG, high * scale + jnp.log(denom), NEG)
            line = jnp.sum(jnp.where(eye_mask(), level, 0.0), axis=0, keepdims=True)
            first = line.astype(jnp.bfloat16)
            rest = line - first.astype(jnp.float32)
            second = rest.astype(jnp.bfloat16)
            third = (rest - second.astype(jnp.float32)).astype(jnp.bfloat16)
            pieces += [first, second, third]
        pieces.append(jnp.zeros((4, HD), jnp.bfloat16))
        for core in range(2):
            o_ref[source * 2 + core, pl.ds(256, 16), :] = jnp.concatenate(pieces, 0)

    def loop(body):
        def step(t, carry):
            body(t)
            return carry

        lax.fori_loop(0, KEY_TILES // GROUP, step, 0)

    prepare(0)
    loop(lambda t: score(0, t))
    for s in range(4):
        settle_high(s)
        if s < 3:
            prepare(s + 1)

        def step(t, s=s):
            weigh(s, t)
            if s < 3:
                score(s + 1, t)

        loop(step)
        close(s)


def attend(plane, slot_frame, radial_mask, queries, cache):
    vmem = pl.BlockSpec(memory_space=pltpu.VMEM)
    smem = pl.BlockSpec(memory_space=pltpu.SMEM)
    square = pltpu.VMEM((4, BLOCK, BLOCK), jnp.float32)
    scores = pltpu.VMEM((4, KEY_TILES, BLOCK, BLOCK), jnp.float32)
    return pl.pallas_call(
        attention_kernel,
        out_shape=jax.ShapeDtypeStruct((8, 272, HD), jnp.bfloat16),
        in_specs=[smem] * 3 + [vmem] * 5,
        out_specs=vmem,
        scratch_shapes=[scores] * 2 + [square] * 4 + [pltpu.VMEM((4 * BLOCK, HD), jnp.float32)],
        cost_estimate=pl.CostEstimate(
            flops=4 * 2048 * 4096 * HD, bytes_accessed=4 * 2**20, transcendentals=2048 * 4096
        ),
        name="attend",
    )(plane, slot_frame, radial_mask, *queries, cache)


def merge_kernel(core_ref, part_ref, out_ref):
    rows = lax.broadcasted_iota(jnp.int32, (64, BLOCK), 0)
    columns = lax.broadcasted_iota(jnp.int32, (64, BLOCK), 1)
    mine = columns == (rows // 16) * 32 + core_ref[0] * 16 + rows % 16
    for head in range(2):
        tails = [part_ref[2 * p + head, pl.ds(256, 16), :].astype(jnp.float32) for p in range(4)]
        for i in range(4):
            levels = [
                tail[3 * i : 3 * i + 1] + tail[3 * i + 1 : 3 * i + 2] + tail[3 * i + 2 : 3 * i + 3]
                for tail in tails
            ]
            high = functools.reduce(jnp.maximum, levels)
            shares = [jnp.exp(level - high) for level in levels]
            whole = functools.reduce(jnp.add, shares)
            summed = jnp.zeros((64, HD), jnp.float32)
            for p in range(4):
                column = jnp.sum(jnp.where(mine, shares[p] / whole, 0.0), axis=1, keepdims=True)
                part = part_ref[2 * p + head, pl.ds(i * 64, 64), :].astype(jnp.float32)
                summed = summed + part * column
            out_ref[pl.ds(i * 64, 64), head * HD : (head + 1) * HD] = summed.astype(jnp.bfloat16)


def merge(core, parts):
    vmem = pl.BlockSpec(memory_space=pltpu.VMEM)
    return pl.pallas_call(
        merge_kernel,
        out_shape=jax.ShapeDtypeStruct((256, 2 * HD), jnp.bfloat16),
        in_specs=[pl.BlockSpec(memory_space=pltpu.SMEM), vmem],
        out_specs=vmem,
        name="merge",
    )(core, parts)


def project_kernel(place_ref, *refs):
    rows, w_ref, out_ref = refs[:4], refs[4], refs[5]
    total = None
    for s in range(4):
        source = lax.rem(place_ref[0] - s + 4, 4)
        w = w_ref[:, pl.ds(pl.multiple_of(source * 256, 256), 256)]
        term = lax.dot_general(rows[s][...], w, NT, preferred_element_type=jnp.float32)
        total = term if total is None else total + term
    for target in range(16):
        out_ref[target] = total[target * Q_DEV : (target + 1) * Q_DEV].astype(jnp.bfloat16)


def project(place, rows, weights):
    vmem = pl.BlockSpec(memory_space=pltpu.VMEM)
    width = weights.shape[0]
    return pl.pallas_call(
        project_kernel,
        out_shape=jax.ShapeDtypeStruct((16, Q_DEV, width), jnp.bfloat16),
        in_specs=[pl.BlockSpec(memory_space=pltpu.SMEM)] + [vmem] * 5,
        out_specs=vmem,
        name="project",
    )(place, *rows, weights)


def pack_query_kernel(place_ref, near_ref, far_ref, *out_refs):
    x, core = place_ref[1], place_ref[2]
    for s in range(4):
        for y in range(4):
            head = y * 8 + lax.rem(x + s, 4) * 2 + core
            columns = pl.ds(pl.multiple_of(head * HD, HD), HD)
            for side, w_ref in enumerate((near_ref, far_ref)):
                out_refs[s][side, :, y * HD : (y + 1) * HD] = w_ref[:, columns]


def pack_query(place, near, far):
    vmem = pl.BlockSpec(memory_space=pltpu.VMEM)
    rows = near.shape[0]
    return pl.pallas_call(
        pack_query_kernel,
        out_shape=(jax.ShapeDtypeStruct((2, rows, 4 * HD), jnp.bfloat16),) * 4,
        in_specs=[pl.BlockSpec(memory_space=pltpu.SMEM), vmem, vmem],
        out_specs=(vmem,) * 4,
        name="pack_query",
    )(place, near, far)


def pack_cache_kernel(k_ref, v_ref, out_ref):
    for head in range(HEADS):
        out_ref[head, :BLOCK, :] = k_ref[:, head * HD : (head + 1) * HD]
        out_ref[head, BLOCK:, :] = v_ref[:, head * HD : (head + 1) * HD]


def pack_cache(keys, values):
    vmem = pl.BlockSpec(memory_space=pltpu.VMEM)
    return pl.pallas_call(
        pack_cache_kernel,
        out_shape=jax.ShapeDtypeStruct((HEADS, 2 * BLOCK, HD), jnp.bfloat16),
        in_specs=[vmem, vmem],
        out_specs=vmem,
        name="pack_cache",
    )(keys, values)


def pack_tokens_kernel(token_ref, out_ref):
    width = out_ref.shape[2]
    for target in range(HEADS):
        column = target // 8 * width
        out_ref[target] = token_ref[:, column : column + width]


def pack_tokens(tokens):
    vmem = pl.BlockSpec(memory_space=pltpu.VMEM)
    return pl.pallas_call(
        pack_tokens_kernel,
        out_shape=jax.ShapeDtypeStruct((HEADS, Q_DEV, tokens.shape[1] // 4), jnp.bfloat16),
        in_specs=[vmem],
        out_specs=vmem,
        name="pack_tokens",
    )(tokens)


def settle_kernel(place_ref, *refs):
    parts, out_ref = refs[:8], refs[8]
    x, zl = place_ref[1], place_ref[3]
    size = parts[0].shape[0]
    for z_side in range(2):
        for s in range(4):
            block = lax.rem(zl + z_side, 2) * 4 + lax.rem(x - s + 4, 4)
            out_ref[pl.ds(pl.multiple_of(block * size, 16), size), :] = parts[z_side * 4 + s][...]


def settle(place, parts):
    vmem = pl.BlockSpec(memory_space=pltpu.VMEM)
    rows, columns = parts[0].shape
    return pl.pallas_call(
        settle_kernel,
        out_shape=jax.ShapeDtypeStruct((8 * rows, columns), jnp.bfloat16),
        in_specs=[pl.BlockSpec(memory_space=pltpu.SMEM)] + [vmem] * 8,
        out_specs=vmem,
        name="settle",
    )(place, *parts)


def finish_kernel(part_ref, out_ref):
    width = part_ref.shape[2]
    for y in range(4):
        parts = [part_ref[y * 4 + x].astype(jnp.float32) for x in range(4)]
        total = functools.reduce(jnp.add, parts)
        out_ref[:, y * width : (y + 1) * width] = total.astype(jnp.bfloat16)


def finish(parts):
    vmem = pl.BlockSpec(memory_space=pltpu.VMEM)
    _, rows, width = parts.shape
    return pl.pallas_call(
        finish_kernel,
        out_shape=jax.ShapeDtypeStruct((rows, 4 * width), jnp.bfloat16),
        in_specs=[vmem],
        out_specs=vmem,
        name="finish",
    )(parts)


def pack_out_kernel(place_ref, w_ref, *out_refs):
    x = place_ref[1]
    for s in range(4):
        for y in range(4):
            head = y * 8 + lax.rem(x + s, 4) * 2
            columns = pl.ds(pl.multiple_of(head * HD, 2 * HD), 2 * HD)
            out_refs[s][:, y * 2 * HD : (y + 1) * 2 * HD] = w_ref[:, columns]


def pack_out(place, table):
    vmem = pl.BlockSpec(memory_space=pltpu.VMEM)
    rows = table.shape[0]
    return pl.pallas_call(
        pack_out_kernel,
        out_shape=(jax.ShapeDtypeStruct((rows, 8 * HD), jnp.bfloat16),) * 4,
        in_specs=[pl.BlockSpec(memory_space=pltpu.SMEM), vmem],
        out_specs=(vmem,) * 4,
        name="pack_out",
    )(place, table)


def weave_query_kernel(place_ref, *refs):
    weights, out_ref = refs[:8], refs[8]
    y, x, core, zl = place_ref[0], place_ref[1], place_ref[2], place_ref[3]
    size = weights[0].shape[1]
    for z_side in range(2):
        for side in range(2):
            for s in range(4):
                block = lax.rem(zl + z_side, 2) * 8 + lax.rem(x - s + 4, 4) * 2
                block = block + lax.rem(core + side, 2)
                rows = pl.ds(pl.multiple_of(block * size, 16), size)
                for t in range(4):
                    columns = pl.ds(pl.multiple_of(lax.rem(y + t, 4) * HD, HD), HD)
                    block = weights[z_side * 4 + s][side, :, columns]
                    out_ref[rows, t * HD : (t + 1) * HD] = block


def weave_query(place, weights):
    vmem = pl.BlockSpec(memory_space=pltpu.VMEM)
    _, rows, columns = weights[0].shape
    return pl.pallas_call(
        weave_query_kernel,
        out_shape=jax.ShapeDtypeStruct((16 * rows, columns), jnp.bfloat16),
        in_specs=[pl.BlockSpec(memory_space=pltpu.SMEM)] + [vmem] * 8,
        out_specs=vmem,
        name="weave_query",
    )(place, *weights)


def weave_out_kernel(place_ref, *refs):
    weights, out_ref = refs[:2], refs[2]
    core = place_ref[2]
    size = weights[0].shape[0] // 8
    for side in range(2):
        for pair in range(8):
            block = pair * 2 + lax.rem(core + side, 2)
            target = pl.ds(pl.multiple_of(block * size, 16), size)
            out_ref[target, :] = weights[side][pl.ds(pair * size, size), :]


def weave_out(place, weights):
    vmem = pl.BlockSpec(memory_space=pltpu.VMEM)
    rows, columns = weights[0].shape
    return pl.pallas_call(
        weave_out_kernel,
        out_shape=jax.ShapeDtypeStruct((2 * rows, columns), jnp.bfloat16),
        in_specs=[pl.BlockSpec(memory_space=pltpu.SMEM)] + [vmem] * 2,
        out_specs=vmem,
        name="weave_out",
    )(place, *weights)


def query_kernel(token_ref, w_ref, *out_refs):
    for pair in range(2):
        w = w_ref[:, pair * 2 * HD : (pair + 1) * 2 * HD]
        total = jnp.dot(token_ref[...], w, preferred_element_type=jnp.float32)
        out_refs[2 * pair][...] = total[:, :HD]
        out_refs[2 * pair + 1][...] = total[:, HD:]


def query_parts(token_rows, weights):
    vmem = pl.BlockSpec(memory_space=pltpu.VMEM)
    rows, depth = token_rows.shape
    return pl.pallas_call(
        query_kernel,
        out_shape=(jax.ShapeDtypeStruct((rows, HD), jnp.float32),) * 4,
        in_specs=[vmem] * 2,
        out_specs=(vmem,) * 4,
        cost_estimate=pl.CostEstimate(
            flops=2 * rows * depth * 4 * HD, bytes_accessed=4 * 2**20, transcendentals=0
        ),
        name="query_parts",
    )(token_rows, weights)


def z_shift(value, shift):
    return lax.ppermute(value, ("tm", "zl"), [(i, (i + shift) % 4) for i in range(4)])


def ring_shift(value, axis, shift):
    return lax.ppermute(value, axis, [(i, (i + shift) % 4) for i in range(4)])


def far_first(parts, axis):
    far = ring_shift(parts[2], axis, 2)
    near = [ring_shift(parts[s], axis, s) for s in (1, 3)]
    return [parts[0], near[0], far, near[1]]


def core_swap(value):
    return lax.ppermute(value, "c", [(0, 1), (1, 0)])


def exchange(table, axes):
    return lax.all_to_all(table, axes, split_axis=0, concat_axis=0, tiled=True)


def on_device(tokens, w_query, w_out, k_cache, v_cache, radial_mask, slot_frame):
    plane = (lax.axis_index("tm") * 2 + lax.axis_index("zl")).reshape(1)
    core = lax.axis_index("c").reshape(1)
    place = jnp.stack([lax.axis_index(a) for a in ("y", "x", "c", "zl")])

    packed = pack_query(place, w_query, core_swap(w_query))
    got = [packed[0]] + [ring_shift(packed[s], "x", s) for s in (1, 2, 3)]
    weights = got + [z_shift(got[s], 1) for s in (0, 1)] + [z_shift(got[s], -1) for s in (2, 3)]

    token_rows = exchange(pack_tokens(tokens), PLANE)

    packed_out = pack_out(place, w_out.T)
    got_out = [packed_out[0]] + [ring_shift(packed_out[s], "x", s) for s in (1, 2, 3)]

    cache = pack_cache(k_cache, v_cache)
    weights = weave_query(place, weights)
    weights, cache, token_rows = lax.optimization_barrier((weights, cache, token_rows))

    partial = query_parts(token_rows.reshape(-1, token_rows.shape[2]), weights)
    partial, cache, got_out = lax.optimization_barrier((partial, cache, got_out))
    partial = far_first(partial, "y")
    arrived = exchange(cache, PLANE)
    got_out = list(got_out)
    got_out += [z_shift(got_out[s], 1) for s in (0, 1)]
    got_out += [z_shift(got_out[s], -1) for s in (2, 3)]

    query = functools.reduce(jnp.add, partial).astype(jnp.bfloat16)
    queries = [query] + [z_shift(query, s) for s in (1, 2, 3)]
    outs = attend(plane, slot_frame, radial_mask, queries, arrived)

    got_out, outs = lax.optimization_barrier((got_out, outs))
    out_near = settle(place, got_out)
    parts = exchange(outs, ("tm", "zl", "c"))
    out_far = core_swap(out_near)
    out_weights = weave_out(place, (out_near, out_far))
    attended = merge(core, parts)
    rows = [attended] + [ring_shift(attended, "y", s) for s in (1, 2, 3)]
    return finish(exchange(project(place, rows, out_weights), ("y", "x")))


def solution(mesh):
    fine = Mesh(mesh.devices.reshape(2, 4, 2, 4, 2), AXES)
    return jax.shard_map(
        on_device,
        mesh=fine,
        in_specs=(
            P(AXES, None),
            P(("y", "zl", "x", "c"), None),
            P(None, ("y", "zl", "x", "c")),
            P(AXES, None),
            P(AXES, None),
            P(),
            P(),
        ),
        out_specs=P(AXES, None),
        check_vma=False,
    )
```
